32 devices in a mesh: dp: 2 (over x), cols: 4 (over z), rows: 4 (over y, core).
Axes of the slice: x: 2, y: 2, z: 4, core: 2. Of those that a mesh axis runs over, the one named last changes fastest.
Arguments:
- h_init: bfloat16 [2, 96, 96, 256], P('dp', 'rows', 'cols'), parts along dimension 0
- c_init: float32 [2, 96, 96, 256], P('dp', 'rows', 'cols'), parts along dimension 0
- w_rec: bfloat16 [3, 3, 256, 1024], replicated
- gate_bias: float32 [24, 1024], replicated
Outputs:
- output 1: bfloat16 [24, 2, 96, 96, 256], P(None, 'dp', 'rows', 'cols'), parts along dimension 1
- output 2: float32 [2, 96, 96, 256], P('dp', 'rows', 'cols'), parts along dimension 0
There are 2 independent parts. The reference program is written for one: setup_inputs(seed, part) draws one part's arguments, and reference() takes and returns one part's arrays. A program takes and returns all parts, laid end to end along the dimension named above; an argument that names none is the same for every part.
All inputs are finite; a program needn't handle non-finite values.
Results may differ from the reference program's by a relative error of at most 0.00408108.
Values are sent between devices in bfloat16 or wider.
A program may use at most 1 GiB of HBM per device.

```python
import jax
import jax.numpy as jnp
from jax import lax

STEPS = 24
BATCH = 1
GRID_H = 96
GRID_W = 96
CHANNELS = 256


def setup_inputs(seed: int = 0, part: int = 0) -> dict:
    key_w, key_b = jax.random.split(jax.random.key(seed))
    part_key = jax.random.fold_in(jax.random.key(seed + 1), part)
    key_h, key_c = jax.random.split(part_key)
    fan_in = 9 * CHANNELS
    w_rec = (jax.random.normal(key_w, (3, 3, CHANNELS, 4 * CHANNELS), jnp.float32) * (1.5 * fan_in ** -0.5)).astype(jnp.bfloat16)
    gate_offset = jnp.repeat(jnp.array([0.0, 1.0, 0.0, 0.0], jnp.float32), CHANNELS)
    gate_bias = jax.random.normal(key_b, (STEPS, 4 * CHANNELS), jnp.float32) * 0.5 + gate_offset
    h_init = (jax.random.normal(key_h, (BATCH, GRID_H, GRID_W, CHANNELS), jnp.float32) * 0.6).astype(jnp.bfloat16)
    c_init = jax.random.normal(key_c, (BATCH, GRID_H, GRID_W, CHANNELS), jnp.float32)
    return {"h_init": h_init, "c_init": c_init, "w_rec": w_rec, "gate_bias": gate_bias}


def reference(h_init, c_init, w_rec, gate_bias):
    w_wide = w_rec.astype(jnp.float32)

    def one_step(carry_in, bias_row):
        h_prev, c_prev = carry_in
        gate_pre = lax.conv_general_dilated(h_prev.astype(jnp.float32), w_wide, (1, 1), "SAME", dimension_numbers=("NHWC", "HWIO", "NHWC")) + bias_row
        in_gate, forget_gate, out_gate, cand_gate = jnp.split(gate_pre, 4, axis=-1)
        c_next = jax.nn.sigmoid(forget_gate) * c_prev + jax.nn.sigmoid(in_gate) * jnp.tanh(cand_gate)
        h_next = (jax.nn.sigmoid(out_gate) * jnp.tanh(c_next)).astype(jnp.bfloat16)
        return (h_next, c_next), h_next

    final_state, h_seq = lax.scan(one_step, (h_init, c_init), gate_bias)
    return h_seq, final_state[1]
```

```python
import functools

import jax
import jax.numpy as jnp
from jax import lax
from jax.experimental import pallas as pl
from jax.experimental.pallas import tpu as pltpu
from jax.sharding import PartitionSpec as P

T = 24
CH = 256
PITCH = 29
ROWS = 34
MESH = pl.DeviceIdType.MESH
DIRS = ((-1, 0), (0, -1), (-1, -1), (-1, 1), (1, -1), (1, 1), (0, 1), (1, 0))


def addr(h, w):
    return 2 * ((h + 2) * PITCH + (w + 2))


def cells(piece, dh=0, dw=0):
    kind, h, w, n = piece
    stride = 2 if kind == "H" else 2 * PITCH
    return pl.ds(addr(h + dh, w + dw), 8 * n, stride=stride)


IN1 = [("V", 1, w, 2) for w in range(1, 23)] + [p for h in range(17, 23) for p in (("H", h, 1, 2), ("H", h, 15, 1))]
RIM1 = [("V", 1, w, 3) for w in (-1, 0, 23, 24)]
RIM1 += [p for h in (-1, 0) for p in (("H", h, -1, 3), ("H", h, 17, 1))]
RIM1 += [p for h in (23, 24) for p in (("H", h, 1, 2), ("H", h, 15, 1))]
RIM2 = [("H", h, 0, 3) for h in (0, 1, 18, 19, 20, 21, 22, 23)] + [("V", 2, w, 2) for w in (0, 1, 22, 23)]
IN2 = [("V", 2, w, 2) for w in range(2, 22)]

TAPS = [(dh, dw) for dh in (-1, 0, 1) for dw in (-1, 0, 1)]
KTILES = [((2 * k, 0), (2 * k + 1, 0)) for k in range(4)] + [((8, 0), (8, 1))]
KTILES += [((2 * k, 1), (2 * k + 1, 1)) for k in range(4)]


def split8(block):
    out = []
    for kind, h, w, n in block:
        for g in range(n):
            out.append((kind, h + 8 * g, w, 1) if kind == "V" else (kind, h, w + 8 * g, 1))
    return out


def kernel(steps, row_count, col_count, h_in, c_in, w_in, bias, h_out, c_out, *scratch):
    (he, ho, ce, co, mask, wts, pack, c_stage, col_send, cor_send, crow_send, ccor_send,
     hline, hcor, cline, ccor, load_sem, out_sem, send_sem, recv_sem) = scratch
    dp = lax.axis_index("dp")
    col = lax.axis_index("cols")
    row = lax.axis_index("rows")

    def has(k):
        dr, dc = DIRS[k]
        ok = jnp.int32(1)
        if dr:
            ok = ok * jnp.where((row > 0) if dr < 0 else (row < row_count - 1), 1, 0)
        if dc:
            ok = ok * jnp.where((col > 0) if dc < 0 else (col < col_count - 1), 1, 0)
        return ok

    present = [has(k) for k in range(8)]

    def target(k):
        dr, dc = DIRS[k]
        ok = present[k]
        return (jnp.where(ok == 1, dp, 1 - dp), col + ok * dc, row + ok * dr), jnp.where(ok == 1, 7 - k, k)

    loads = []
    for p in range(2):
        for gate in range(4):
            loads.append(pltpu.make_async_copy(
                w_in.at[:, :, pl.ds(gate * CH + p * 128, 128)],
                wts.at[p, :, :, pl.ds(gate * 128, 128)], load_sem.at[2 + p * 4 + gate]))
    h_load = pltpu.make_async_copy(h_in, pack.at[1], load_sem.at[0])
    c_load = pltpu.make_async_copy(c_in, c_stage, load_sem.at[1])
    h_load.start()
    c_load.start()
    for ld in loads:
        ld.start()

    barrier = pltpu.get_barrier_semaphore()
    for k in range(8):
        dev, _ = target(k)
        pl.semaphore_signal(barrier, inc=1, device_id=dev, device_id_type=MESH)

    hmin, hmax = -present[0], T - 1 + present[7]
    wmin, wmax = -present[1], T - 1 + present[6]
    for piece in split8(RIM1):
        kind, h, w, _ = piece
        line = lax.broadcasted_iota(jnp.int32, (8, 128), 0)
        hh = line + h if kind == "V" else jnp.full((8, 128), h, jnp.int32)
        ww = line + w if kind == "H" else jnp.full((8, 128), w, jnp.int32)
        inside = (hh >= hmin) & (hh <= hmax) & (ww >= wmin) & (ww <= wmax)
        mask[cells(piece), :] = jnp.where(inside, 1.0, 0.0)

    h_load.wait()
    for h in range(0, T, 2):
        val = pack[1, pl.ds(h * T, 2 * T), :].astype(jnp.float32)
        for s in range(2):
            for p in range(2):
                he[p][cells(("H", h + s, 0, 3)), :] = val[s * T:(s + 1) * T, p * 128:(p + 1) * 128]
    c_load.wait()
    for h in range(T):
        for p in range(2):
            ce[p][cells(("H", h, 0, 3)), :] = c_stage[pl.ds(h * T, T), pl.ds(p * 128, 128)]

    def both(bufs, piece):
        return jnp.concatenate([bufs[0][cells(piece), :], bufs[1][cells(piece), :]], axis=1)

    def pack_rows(bufs, slot, h):
        val = jnp.concatenate([both(bufs, ("H", h, 0, 3)), both(bufs, ("H", h + 1, 0, 3))], axis=0)
        pack[slot, pl.ds(h * T, 2 * T), :] = val.astype(jnp.bfloat16)

    def pack_sends():
        for j, w in enumerate((0, 22)):
            val = jnp.concatenate([both(he, ("V", 0, w, 3)), both(he, ("V", 0, w + 1, 3))], axis=0)
            col_send[j] = val.astype(jnp.bfloat16)
        for j, (h, w) in enumerate(((0, 0), (0, 22), (22, 0), (22, 22))):
            val = jnp.concatenate([both(he, ("V", h, w, 1)), both(he, ("V", h, w + 1, 1))], axis=0)
            cor_send[j] = val.astype(jnp.bfloat16)
        for j, piece in enumerate((("H", 0, 0, 3), ("V", 0, 0, 3), ("V", 0, 23, 3), ("H", 23, 0, 3))):
            crow_send[j] = both(ce, piece)
        for j, (h, w) in enumerate(((0, 0), (0, 23), (23, 0), (23, 23))):
            ccor_send[j] = both(ce, ("V", h, w, 1))

    def copy(k, n, slot, dev, there):
        dr, dc = DIRS[k]
        if dr and dc:
            j = (0 if dr < 0 else 2) + (0 if dc < 0 else 1)
            pairs = ((cor_send.at[j], hcor.at[slot, there]), (ccor_send.at[j], ccor.at[slot, there]))
        else:
            j = {0: 0, 1: 1, 6: 2, 7: 3}[k]
            if dr:
                src = pack.at[1, pl.ds(0 if dr < 0 else (T - 2) * T, 2 * T)]
            else:
                src = col_send.at[0 if dc < 0 else 1]
            pairs = ((src, hline.at[slot, there]), (crow_send.at[j], cline.at[slot, there]))
        return pltpu.make_async_remote_copy(
            src_ref=pairs[n][0], dst_ref=pairs[n][1], send_sem=send_sem.at[k, n],
            recv_sem=recv_sem.at[slot, there, n], device_id=dev, device_id_type=MESH)

    ORDER = (2, 3, 4, 5, 1, 6, 0, 7)

    def start_sends(slot):
        for n in range(2):
            for k in ORDER:
                dev, there = target(k)
                copy(k, n, slot, dev, there).start()

    def wait_sends(slot):
        for k in range(8):
            dev, there = target(k)
            for n in range(2):
                copy(k, n, slot, dev, there).wait_send()

    def wait_recvs(slot):
        for k in range(8):
            dev, _ = target(k)
            for n in range(2):
                copy(7 - k, n, slot, dev, k).wait_recv()

    def unpack(slot):
        for k in range(8):
            dr, dc = DIRS[k]
            ok = present[k] == 1
            if dr and dc:
                val = jnp.where(ok, hcor[slot, k].astype(jnp.float32), 0.0)
                h, w = (-2 if dr < 0 else T), (-2 if dc < 0 else T)
                for s in range(2):
                    for p in range(2):
                        he[p][pl.ds(addr(h, w + s), 2, stride=2 * PITCH), :] = val[8 * s:8 * s + 2, p * 128:(p + 1) * 128]
                cval = ccor[slot, k]
                h, w = (-1 if dr < 0 else T), (-1 if dc < 0 else T)
                for p in range(2):
                    ce[p][pl.ds(addr(h, w), 1), :] = cval[0:1, p * 128:(p + 1) * 128]
            else:
                val = jnp.where(ok, hline[slot, k].astype(jnp.float32), 0.0)
                cval = cline[slot, k]
                for s in range(2):
                    piece = ("H", (-2 if dr < 0 else T) + s, 0, 3) if dr else ("V", 0, (-2 if dc < 0 else T) + s, 3)
                    for p in range(2):
                        he[p][cells(piece), :] = val[s * T:(s + 1) * T, p * 128:(p + 1) * 128]
                piece = ("H", -1 if dr < 0 else T, 0, 3) if dr else ("V", 0, -1 if dc < 0 else T, 3)
                for p in range(2):
                    ce[p][cells(piece), :] = cval[:, p * 128:(p + 1) * 128]

    pack_sends()
    pl.semaphore_wait(barrier, 8)
    start_sends(0)
    for ld in loads:
        ld.wait()

    def rhs(p, k):
        parts = [wts[p, tap, pl.ds(half * 128, 128), :] for tap, half in KTILES[k]]
        return jnp.concatenate(parts, axis=0)

    def lhs_of(bufs, block, k):
        parts = []
        for tap, half in KTILES[k]:
            dh, dw = TAPS[tap]
            parts.append(jnp.concatenate([bufs[half][cells(piece, dh, dw), :] for piece in block], axis=0))
        return jnp.concatenate(parts, axis=1).astype(jnp.bfloat16)

    def epilogue(i, p, pair, gates, c_src, c_dst, h_dst, step_bias, masked):
        b_i, b_f, b_o, b_g = (step_bias[gate * 2 + p] for gate in range(4))
        for s, piece in enumerate(pair):
            v = gates[16 * i + 8 * s:16 * i + 8 * s + 8]
            in_gate = 0.5 * jnp.tanh(0.5 * (v[:, :128] + b_i)) + 0.5
            forget = 0.5 * jnp.tanh(0.5 * (v[:, 128:256] + b_f)) + 0.5
            out_gate = 0.5 * jnp.tanh(0.5 * (v[:, 256:384] + b_o)) + 0.5
            cand = jnp.tanh(v[:, 384:] + b_g)
            c_new = forget * c_src[p][cells(piece), :] + in_gate * cand
            c_dst[p][cells(piece), :] = c_new
            h_new = (out_gate * jnp.tanh(c_new)).astype(jnp.bfloat16).astype(jnp.float32)
            if masked:
                h_new = h_new * mask[cells(piece), :]
            h_dst[p][cells(piece), :] = h_new

    def pair_steps(n, _):
        slot = lax.rem(n, 2)
        biases = []
        for s in range(2):
            line = bias[pl.ds(2 * n + s, 1), :]
            biases.append([jnp.broadcast_to(line[:, j * 128:(j + 1) * 128], (8, 128)) for j in range(8)])
        first = (he, ho, ce, co, biases[0])
        second = (ho, he, co, ce, biases[1])
        plan = [(IN1, first, False), (RIM1, first, True), (RIM2, second, False), (IN2, second, False)]
        stages = [(b, p) for b in range(4) for p in range(2)]
        odd_out = pltpu.make_async_copy(pack.at[0], h_out.at[2 * n], out_sem.at[0])
        even_out = pltpu.make_async_copy(pack.at[1], h_out.at[2 * n + 1], out_sem.at[1])
        todo = []
        for idx, (b, p) in enumerate(stages):
            block, (src, h_dst, c_src, c_dst, step_bias), masked = plan[b]
            groups = split8(block)
            if (b, p) == (1, 0):
                wait_recvs(slot)
                unpack(slot)
            if (b, p) == (2, 1):
                @pl.when(n > 0)
                def _():
                    odd_out.wait()
            per_tile = -(-len(todo) // 4)
            gates = None
            for k in range(9):
                part = jnp.dot(lhs_of(src, block, k), rhs(p, k), preferred_element_type=jnp.float32)
                gates = part if gates is None else gates + part
                for unit in todo[:per_tile]:
                    unit()
                todo = todo[per_tile:]
                if (b, p) == (2, 1) and k >= 3:
                    for h in range(4 * (k - 3), min(4 * (k - 3) + 4, T), 2):
                        pack_rows(ho, 0, h)
                if (b, p) == (3, 0) and k == 4:
                    odd_out.start()
                    @pl.when(n > 0)
                    def _():
                        even_out.wait()
                    wait_sends(slot)
                    pack_rows(he, 1, 0)
                    pack_rows(he, 1, T - 2)
                    pack_sends()
                    start_sends(1 - slot)
            todo = [functools.partial(epilogue, i, p, groups[2 * i:2 * i + 2], gates, c_src, c_dst, h_dst, step_bias, masked)
                    for i in range(len(groups) // 2)]
        for unit in todo:
            unit()
        for h in range(2, T - 2, 2):
            pack_rows(he, 1, h)
        even_out.start()
        return 0

    lax.fori_loop(0, steps // 2, pair_steps, 0)

    for h in range(T):
        c_stage[pl.ds(h * T, T), :] = both(ce, ("H", h, 0, 3))
    c_save = pltpu.make_async_copy(c_stage, c_out, load_sem.at[1])
    c_save.start()
    last = steps // 2
    wait_recvs(last % 2)
    wait_sends(last % 2)
    for s in range(2):
        pltpu.make_async_copy(pack.at[s], h_out.at[steps - 2 + s], out_sem.at[s]).wait()
    c_save.wait()


def solution(mesh):
    row_count = mesh.shape["rows"]
    col_count = mesh.shape["cols"]
    assert mesh.shape["dp"] == 2

    def device_fn(h_init, c_init, w_rec, gate_bias):
        steps = gate_bias.shape[0]
        assert h_init.shape == (1, T, T, CH) and steps % 2 == 0
        cell_rows = 2 * ROWS * PITCH
        f32, bf16 = jnp.float32, jnp.bfloat16
        plane = [pltpu.VMEM((cell_rows, 128), f32)] * 2
        hbm = pl.BlockSpec(memory_space=pl.ANY)
        scratch = [
            plane, plane, plane, plane,
            pltpu.VMEM((cell_rows, 128), f32),
            pltpu.VMEM((2, 9, 256, 512), bf16),
            pltpu.VMEM((2, T * T, CH), bf16),
            pltpu.VMEM((T * T, CH), f32),
            pltpu.VMEM((2, 2 * T, CH), bf16),
            pltpu.VMEM((4, 16, CH), bf16),
            pltpu.VMEM((4, T, CH), f32),
            pltpu.VMEM((4, 8, CH), f32),
            pltpu.VMEM((2, 8, 2 * T, CH), bf16),
            pltpu.VMEM((2, 8, 16, CH), bf16),
            pltpu.VMEM((2, 8, T, CH), f32),
            pltpu.VMEM((2, 8, 8, CH), f32),
            pltpu.SemaphoreType.DMA((10,)),
            pltpu.SemaphoreType.DMA((2,)),
            pltpu.SemaphoreType.DMA((8, 2)),
            pltpu.SemaphoreType.DMA((2, 8, 2)),
        ]
        flat, shapes = [], []
        for s in scratch:
            shapes.append(len(s) if isinstance(s, list) else 0)
            flat += s if isinstance(s, list) else [s]

        def body(*refs):
            args, rest = refs[:6], list(refs[6:])
            grouped = []
            for count in shapes:
                if count:
                    grouped.append([rest.pop(0) for _ in range(count)])
                else:
                    grouped.append(rest.pop(0))
            kernel(steps, row_count, col_count, *args, *grouped)

        h_seq, c_last = pl.pallas_call(
            body,
            out_shape=(jax.ShapeDtypeStruct((steps, T * T, CH), bf16), jax.ShapeDtypeStruct((T * T, CH), f32)),
            in_specs=[hbm, hbm, hbm, pl.BlockSpec(memory_space=pltpu.VMEM)],
            out_specs=(hbm, hbm),
            scratch_shapes=flat,
            compiler_params=pltpu.CompilerParams(collective_id=0, has_side_effects=True, vmem_limit_bytes=48 * 1024 * 1024),
            name="conv_lstm",
        )(h_init.reshape(T * T, CH), c_init.reshape(T * T, CH), w_rec.reshape(9, CH, 4 * CH), gate_bias)
        return h_seq.reshape(steps, 1, T, T, CH), c_last.reshape(1, T, T, CH)

    state_spec = P("dp", "rows", "cols", None)
    return jax.shard_map(device_fn, mesh=mesh, in_specs=(state_spec, state_spec, P(), P()), out_specs=(P(None, "dp", "rows", "cols", None), state_spec), check_vma=False)
```

```python
import functools

import jax
import jax.numpy as jnp
from jax import lax
from jax.experimental import pallas as pl
from jax.experimental.pallas import tpu as pltpu
from jax.sharding import PartitionSpec as P

T = 24
CH = 256
PITCH = 29
ROWS = 34
MESH = pl.DeviceIdType.MESH
DIRS = ((-1, 0), (0, -1), (-1, -1), (-1, 1), (1, -1), (1, 1), (0, 1), (1, 0))


def addr(h, w):
    return 2 * ((h + 2) * PITCH + (w + 2))


def cells(piece, dh=0, dw=0):
    kind, h, w, n = piece
    stride = 2 if kind == "H" else 2 * PITCH
    return pl.ds(addr(h + dh, w + dw), 8 * n, stride=stride)


IN1 = [("V", 1, w, 2) for w in range(1, 23)] + [p for h in range(17, 23) for p in (("H", h, 1, 2), ("H", h, 15, 1))]
RIM1 = [("V", 1, w, 3) for w in (-1, 0, 23, 24)]
RIM1 += [p for h in (-1, 0) for p in (("H", h, -1, 3), ("H", h, 17, 1))]
RIM1 += [p for h in (23, 24) for p in (("H", h, 1, 2), ("H", h, 15, 1))]
RIM2 = [("H", h, 0, 3) for h in (0, 1, 18, 19, 20, 21, 22, 23)] + [("V", 2, w, 2) for w in (0, 1, 22, 23)]
IN2 = [("V", 2, w, 2) for w in range(2, 22)]

TAPS = [(dh, dw) for dh in (-1, 0, 1) for dw in (-1, 0, 1)]
KTILES = [((2 * k, 0), (2 * k + 1, 0)) for k in range(4)] + [((8, 0), (8, 1))]
KTILES += [((2 * k, 1), (2 * k + 1, 1)) for k in range(4)]


def split8(block):
    out = []
    for kind, h, w, n in block:
        for g in range(n):
            out.append((kind, h + 8 * g, w, 1) if kind == "V" else (kind, h, w + 8 * g, 1))
    return out


def kernel(steps, row_count, col_count, h_in, c_in, w_in, bias_in, h_out, c_out, *scratch):
    (he, hr, ho, ce, co, mask, wts, bias, h_stage, c_stage, row_send, col_send, cline_send, cor_send,
     hline, cline, corner, load_sem, send_sem, recv_sem) = scratch
    dp = lax.axis_index("dp")
    col = lax.axis_index("cols")
    row = lax.axis_index("rows")

    def has(k):
        dr, dc = DIRS[k]
        ok = jnp.int32(1)
        if dr:
            ok = ok * jnp.where((row > 0) if dr < 0 else (row < row_count - 1), 1, 0)
        if dc:
            ok = ok * jnp.where((col > 0) if dc < 0 else (col < col_count - 1), 1, 0)
        return ok

    present = [has(k) for k in range(8)]

    def target(k):
        dr, dc = DIRS[k]
        ok = present[k]
        return (jnp.where(ok == 1, dp, 1 - dp), col + ok * dc, row + ok * dr), jnp.where(ok == 1, 7 - k, k)

    loads = []
    for p in range(2):
        for gate in range(4):
            loads.append(pltpu.make_async_copy(
                w_in.at[:, :, pl.ds(gate * CH + p * 128, 128)],
                wts.at[p, :, :, pl.ds(gate * 128, 128)], load_sem.at[2 + p * 4 + gate]))
    h_load = pltpu.make_async_copy(h_in, h_stage, load_sem.at[0])
    c_load = pltpu.make_async_copy(c_in, c_stage, load_sem.at[1])
    loads.append(pltpu.make_async_copy(bias_in, bias, load_sem.at[10]))
    h_load.start()
    c_load.start()
    for ld in loads:
        ld.start()

    barrier = pltpu.get_barrier_semaphore()
    for k in range(8):
        dev, _ = target(k)
        pl.semaphore_signal(barrier, inc=1, device_id=dev, device_id_type=MESH)

    hmin, hmax = -present[0], T - 1 + present[7]
    wmin, wmax = -present[1], T - 1 + present[6]
    for piece in split8(RIM1):
        kind, h, w, _ = piece
        line = lax.broadcasted_iota(jnp.int32, (8, 128), 0)
        hh = line + h if kind == "V" else jnp.full((8, 128), h, jnp.int32)
        ww = line + w if kind == "H" else jnp.full((8, 128), w, jnp.int32)
        inside = (hh >= hmin) & (hh <= hmax) & (ww >= wmin) & (ww <= wmax)
        mask[cells(piece), :] = jnp.where(inside, 1.0, 0.0)

    h_load.wait()
    for h in range(0, T, 2):
        val = h_stage[pl.ds(h * T, 2 * T), :].astype(jnp.float32)
        for s in range(2):
            for p in range(2):
                part = val[s * T:(s + 1) * T, p * 128:(p + 1) * 128]
                he[p][cells(("H", h + s, 0, 3)), :] = part
                hr[p][cells(("H", h + s, 0, 3)), :] = part
    c_load.wait()
    for h in range(T):
        for p in range(2):
            ce[p][cells(("H", h, 0, 3)), :] = c_stage[pl.ds(h * T, T), pl.ds(p * 128, 128)]

    def both(bufs, piece):
        return jnp.concatenate([bufs[0][cells(piece), :], bufs[1][cells(piece), :]], axis=1)

    def two_lines(bufs, first, second):
        return jnp.concatenate([both(bufs, first), both(bufs, second)], axis=0).astype(jnp.bfloat16)

    def pack_rows(bufs, t, h):
        h_out[t, pl.ds(h * T, 2 * T), :] = two_lines(bufs, ("H", h, 0, 3), ("H", h + 1, 0, 3))

    def pack_sends():
        for j, h in enumerate((0, 22)):
            row_send[j] = two_lines(hr, ("H", h, 0, 3), ("H", h + 1, 0, 3))
        for j, w in enumerate((0, 22)):
            col_send[j] = two_lines(hr, ("V", 0, w, 3), ("V", 0, w + 1, 3))
        for j, (h, w) in enumerate(((0, 0), (0, 22), (22, 0), (22, 22))):
            for p in range(2):
                lanes = pl.ds(p * 128, 128)
                for s in range(2):
                    cor_send[j, pl.ds(2 * s, 2), lanes] = hr[p][pl.ds(addr(h, w + s), 2, stride=2 * PITCH), :]
                cor_send[j, pl.ds(4, 1), lanes] = ce[p][pl.ds(addr(h and T - 1, w and T - 1), 1), :]
        for j, piece in enumerate((("H", 0, 0, 3), ("V", 0, 0, 3), ("V", 0, 23, 3), ("H", 23, 0, 3))):
            cline_send[j] = both(ce, piece)

    LINES = (1, 6, 0, 7)
    CORNERS = (2, 3, 4, 5)
    MESSAGES = [(k, 0) for k in CORNERS + LINES] + [(k, 1) for k in LINES]

    def copy(k, n, slot, dev, there):
        dr, dc = DIRS[k]
        if dr and dc:
            src, dst = cor_send.at[(0 if dr < 0 else 2) + (0 if dc < 0 else 1)], corner.at[slot, there]
        elif n:
            src, dst = cline_send.at[{0: 0, 1: 1, 6: 2, 7: 3}[k]], cline.at[slot, there]
        else:
            src, dst = (row_send.at[0 if dr < 0 else 1] if dr else col_send.at[0 if dc < 0 else 1]), hline.at[slot, there]
        return pltpu.make_async_remote_copy(
            src_ref=src, dst_ref=dst, send_sem=send_sem.at[k, n], recv_sem=recv_sem.at[slot, there, n],
            device_id=dev, device_id_type=MESH)

    def start_sends(slot):
        for k, n in MESSAGES:
            dev, there = target(k)
            copy(k, n, slot, dev, there).start()

    def wait_sends(slot):
        for k, n in MESSAGES:
            dev, there = target(k)
            copy(k, n, slot, dev, there).wait_send()

    def wait_recvs(slot, part):
        for k, n in MESSAGES:
            if n == part:
                dev, _ = target(k)
                copy(7 - k, n, slot, dev, k).wait_recv()

    def unpack_h(slot):
        for k in range(8):
            dr, dc = DIRS[k]
            ok = present[k] == 1
            if dr and dc:
                val = jnp.where(ok, corner[slot, k], 0.0)
                h, w = (-2 if dr < 0 else T), (-2 if dc < 0 else T)
                for s in range(2):
                    for p in range(2):
                        hr[p][pl.ds(addr(h, w + s), 2, stride=2 * PITCH), :] = val[2 * s:2 * s + 2, p * 128:(p + 1) * 128]
            else:
                val = jnp.where(ok, hline[slot, k].astype(jnp.float32), 0.0)
                for s in range(2):
                    piece = ("H", (-2 if dr < 0 else T) + s, 0, 3) if dr else ("V", 0, (-2 if dc < 0 else T) + s, 3)
                    for p in range(2):
                        hr[p][cells(piece), :] = val[s * T:(s + 1) * T, p * 128:(p + 1) * 128]

    def unpack_c(slot):
        for k in range(8):
            dr, dc = DIRS[k]
            h, w = (-1 if dr < 0 else T), (-1 if dc < 0 else T)
            for p in range(2):
                lanes = pl.ds(p * 128, 128)
                if dr and dc:
                    ce[p][pl.ds(addr(h, w), 1), :] = corner[slot, k, pl.ds(4, 1), lanes]
                else:
                    piece = ("H", h, 0, 3) if dr else ("V", 0, w, 3)
                    ce[p][cells(piece), :] = cline[slot, k, :, lanes]

    pack_sends()
    pl.semaphore_wait(barrier, 8)
    start_sends(0)
    for ld in loads:
        ld.wait()

    def rhs(p, k):
        parts = [wts[p, tap, pl.ds(half * 128, 128), :] for tap, half in KTILES[k]]
        return jnp.concatenate(parts, axis=0)

    def lhs_of(bufs, block, k):
        parts = []
        for tap, half in KTILES[k]:
            dh, dw = TAPS[tap]
            parts.append(jnp.concatenate([bufs[half][cells(piece, dh, dw), :] for piece in block], axis=0))
        return jnp.concatenate(parts, axis=1).astype(jnp.bfloat16)

    def epilogue(i, p, pair, gates, c_src, c_dst, h_dst, step_bias, rim):
        b_i, b_f, b_o, b_g = (step_bias[gate * 2 + p] for gate in range(4))
        for s, piece in enumerate(pair):
            v = gates[16 * i + 8 * s:16 * i + 8 * s + 8]
            in_gate = 0.5 * jnp.tanh(0.5 * (v[:, :128] + b_i)) + 0.5
            forget = 0.5 * jnp.tanh(0.5 * (v[:, 128:256] + b_f)) + 0.5
            out_gate = 0.5 * jnp.tanh(0.5 * (v[:, 256:384] + b_o)) + 0.5
            cand = jnp.tanh(v[:, 384:] + b_g)
            c_new = forget * c_src[p][cells(piece), :] + in_gate * cand
            c_dst[p][cells(piece), :] = c_new
            h_new = (out_gate * jnp.tanh(c_new)).astype(jnp.bfloat16).astype(jnp.float32)
            if rim == 1:
                h_new = h_new * mask[cells(piece), :]
            h_dst[p][cells(piece), :] = h_new
            if rim == 2 and (piece[0] == "V" or piece[1] in (0, 1, 22, 23) or piece[2] in (0, 16)):
                hr[p][cells(piece), :] = h_new

    def pair_steps(n, _):
        slot = lax.rem(n, 2)
        biases = []
        for s in range(2):
            line = bias[pl.ds(2 * n + s, 1), :]
            biases.append([jnp.broadcast_to(line[:, j * 128:(j + 1) * 128], (8, 128)) for j in range(8)])
        first = (ho, ce, co, biases[0])
        second = (he, co, ce, biases[1])
        plan = [(IN1, he, first, 0), (RIM1, hr, first, 1), (RIM2, ho, second, 2), (IN2, ho, second, 0)]
        todo = []
        for b, p in ((b, p) for b in range(4) for p in range(2)):
            block, src, (h_dst, c_src, c_dst, step_bias), rim = plan[b]
            groups = split8(block)
            per_tile = -(-len(todo) // 4)
            gates = None
            for k in range(9):
                part = jnp.dot(lhs_of(src, block, k), rhs(p, k), preferred_element_type=jnp.float32)
                gates = part if gates is None else gates + part
                for unit in todo[:per_tile]:
                    unit()
                todo = todo[per_tile:]
                if (b, p, k) == (0, 1, 7):
                    wait_recvs(slot, 0)
                    unpack_h(slot)
                if (b, p, k) == (1, 0, 5):
                    wait_recvs(slot, 1)
                    unpack_c(slot)
                if (b, p) == (2, 1) and k >= 3:
                    for h in range(4 * (k - 3), min(4 * (k - 3) + 4, T), 2):
                        pack_rows(ho, 2 * n, h)
                if (b, p, k) == (3, 0, 4):
                    wait_sends(slot)
                    pack_sends()

                    @pl.when(n < steps // 2 - 1)
                    def _():
                        start_sends(1 - slot)
            todo = [functools.partial(epilogue, i, p, groups[2 * i:2 * i + 2], gates, c_src, c_dst, h_dst, step_bias, rim)
                    for i in range(len(groups) // 2)]
        for unit in todo:
            unit()
        for h in range(0, T, 2):
            pack_rows(he, 2 * n + 1, h)
        return 0

    lax.fori_loop(0, steps // 2, pair_steps, 0)

    for h in range(T):
        c_stage[pl.ds(h * T, T), :] = both(ce, ("H", h, 0, 3))
    c_save = pltpu.make_async_copy(c_stage, c_out, load_sem.at[1])
    c_save.start()
    c_save.wait()


def solution(mesh):
    row_count = mesh.shape["rows"]
    col_count = mesh.shape["cols"]
    assert mesh.shape["dp"] == 2

    def device_fn(h_init, c_init, w_rec, gate_bias):
        steps = gate_bias.shape[0]
        assert h_init.shape == (1, T, T, CH) and steps % 2 == 0
        cell_rows = 2 * ROWS * PITCH
        f32, bf16 = jnp.float32, jnp.bfloat16
        plane = [pltpu.VMEM((cell_rows, 128), f32)] * 2
        hbm = pl.BlockSpec(memory_space=pltpu.HBM)
        vmem = pl.BlockSpec(memory_space=pltpu.VMEM)
        scratch = [
            plane, plane, plane, plane, plane,
            pltpu.VMEM((cell_rows, 128), f32),
            pltpu.VMEM((2, 9, 256, 512), bf16),
            pltpu.VMEM((steps, 4 * CH), f32),
            pltpu.VMEM((T * T, CH), bf16),
            pltpu.VMEM((T * T, CH), f32),
            pltpu.VMEM((2, 2 * T, CH), bf16),
            pltpu.VMEM((2, 2 * T, CH), bf16),
            pltpu.VMEM((4, T, CH), f32),
            pltpu.VMEM((4, 8, CH), f32),
            pltpu.VMEM((2, 8, 2 * T, CH), bf16),
            pltpu.VMEM((2, 8, T, CH), f32),
            pltpu.VMEM((2, 8, 8, CH), f32),
            pltpu.SemaphoreType.DMA((11,)),
            pltpu.SemaphoreType.DMA((8, 2)),
            pltpu.SemaphoreType.DMA((2, 8, 2)),
        ]
        flat, shapes = [], []
        for s in scratch:
            shapes.append(len(s) if isinstance(s, list) else 0)
            flat += s if isinstance(s, list) else [s]

        def body(*refs):
            args, rest = refs[:6], list(refs[6:])
            grouped = []
            for count in shapes:
                if count:
                    grouped.append([rest.pop(0) for _ in range(count)])
                else:
                    grouped.append(rest.pop(0))
            kernel(steps, row_count, col_count, *args, *grouped)

        h_seq, c_last = pl.pallas_call(
            body,
            out_shape=(jax.ShapeDtypeStruct((steps, T * T, CH), bf16), jax.ShapeDtypeStruct((T * T, CH), f32)),
            in_specs=[hbm] * 4,
            out_specs=(vmem, hbm),
            scratch_shapes=flat,
            compiler_params=pltpu.CompilerParams(collective_id=0, has_side_effects=True, vmem_limit_bytes=40 * 1024 * 1024),
            name="conv_lstm",
        )(*(pltpu.with_memory_space_constraint(x, pltpu.HBM) for x in (h_init.reshape(T * T, CH), c_init.reshape(T * T, CH), w_rec.reshape(9, CH, 4 * CH), gate_bias)))
        return h_seq.reshape(steps, 1, T, T, CH), c_last.reshape(1, T, T, CH)

    state_spec = P("dp", "rows", "cols", None)
    return jax.shard_map(device_fn, mesh=mesh, in_specs=(state_spec, state_spec, P(), P()), out_specs=(P(None, "dp", "rows", "cols", None), state_spec), check_vma=False)
```

```python
import functools

import jax
import jax.numpy as jnp
from jax import lax
from jax.experimental import pallas as pl
from jax.experimental.pallas import tpu as pltpu
from jax.sharding import PartitionSpec as P

T = 24
CH = 256
PITCH = 29
ROWS = 34
UNROLL = 1
MESH = pl.DeviceIdType.MESH
DIRS = ((-1, 0), (0, -1), (-1, -1), (-1, 1), (1, -1), (1, 1), (0, 1), (1, 0))


def addr(h, w):
    return 2 * ((h + 2) * PITCH + (w + 2))


def cells(piece, dh=0, dw=0):
    kind, h, w, n = piece
    stride = 2 if kind == "H" else 2 * PITCH
    return pl.ds(addr(h + dh, w + dw), 8 * n, stride=stride)


IN1 = [("V", 1, w, 2) for w in range(1, 23)] + [p for h in range(17, 23) for p in (("H", h, 1, 2), ("H", h, 15, 1))]
RIM1 = [("V", 1, w, 3) for w in (-1, 0, 23, 24)]
RIM1 += [p for h in (-1, 0) for p in (("H", h, -1, 3), ("H", h, 17, 1))]
RIM1 += [p for h in (23, 24) for p in (("H", h, 1, 2), ("H", h, 15, 1))]
RIM2 = [("H", h, 0, 3) for h in (0, 1, 18, 19, 20, 21, 22, 23)] + [("V", 2, w, 2) for w in (0, 1, 22, 23)]
IN2 = [("V", 2, w, 2) for w in range(2, 22)]

TAPS = [(dh, dw) for dh in (-1, 0, 1) for dw in (-1, 0, 1)]
KTILES = [((2 * k, 0), (2 * k + 1, 0)) for k in range(4)] + [((8, 0), (8, 1))]
KTILES += [((2 * k, 1), (2 * k + 1, 1)) for k in range(4)]


def split8(block):
    out = []
    for kind, h, w, n in block:
        for g in range(n):
            out.append((kind, h + 8 * g, w, 1) if kind == "V" else (kind, h, w + 8 * g, 1))
    return out


def kernel(steps, row_count, col_count, h_in, c_in, w_in, bias_in, h_out, c_out, *scratch):
    (he, hr, ho, ce, co, mask, wts, bias, h_stage, c_stage, line_send, cline_send, cor_send,
     hline, cline, corner, load_sem, send_sem, recv_sem) = scratch
    dp = lax.axis_index("dp")
    col = lax.axis_index("cols")
    row = lax.axis_index("rows")

    def has(k):
        dr, dc = DIRS[k]
        ok = jnp.int32(1)
        if dr:
            ok = ok * jnp.where((row > 0) if dr < 0 else (row < row_count - 1), 1, 0)
        if dc:
            ok = ok * jnp.where((col > 0) if dc < 0 else (col < col_count - 1), 1, 0)
        return ok

    present = [has(k) for k in range(8)]

    def target(k):
        dr, dc = DIRS[k]
        ok = present[k]
        return (jnp.where(ok == 1, dp, 1 - dp), col + ok * dc, row + ok * dr), ok == 1

    loads = []
    for p in range(2):
        for gate in range(4):
            loads.append(pltpu.make_async_copy(
                w_in.at[:, :, pl.ds(gate * CH + p * 128, 128)],
                wts.at[p, :, :, pl.ds(gate * 128, 128)], load_sem.at[2 + p * 4 + gate]))
    h_load = pltpu.make_async_copy(h_in, h_stage, load_sem.at[0])
    c_load = pltpu.make_async_copy(c_in, c_stage, load_sem.at[1])
    loads.append(pltpu.make_async_copy(bias_in, bias, load_sem.at[10]))
    h_load.start()
    c_load.start()
    for ld in loads:
        ld.start()

    barrier = pltpu.get_barrier_semaphore()
    for k in range(8):
        dev, _ = target(k)
        pl.semaphore_signal(barrier, inc=1, device_id=dev, device_id_type=MESH)

    hmin, hmax = -present[0], T - 1 + present[7]
    wmin, wmax = -present[1], T - 1 + present[6]
    for piece in split8(RIM1):
        kind, h, w, _ = piece
        line = lax.broadcasted_iota(jnp.int32, (8, 128), 0)
        hh = line + h if kind == "V" else jnp.full((8, 128), h, jnp.int32)
        ww = line + w if kind == "H" else jnp.full((8, 128), w, jnp.int32)
        inside = (hh >= hmin) & (hh <= hmax) & (ww >= wmin) & (ww <= wmax)
        mask[cells(piece), :] = jnp.where(inside, 1.0, 0.0)

    h_load.wait()
    for h in range(0, T, 2):
        val = h_stage[pl.ds(h * T, 2 * T), :].astype(jnp.float32)
        for s in range(2):
            for p in range(2):
                part = val[s * T:(s + 1) * T, p * 128:(p + 1) * 128]
                he[p][cells(("H", h + s, 0, 3)), :] = part
                hr[p][cells(("H", h + s, 0, 3)), :] = part
    c_load.wait()
    for h in range(T):
        for p in range(2):
            ce[p][cells(("H", h, 0, 3)), :] = c_stage[pl.ds(h * T, T), pl.ds(p * 128, 128)]

    def both(bufs, piece):
        return jnp.concatenate([bufs[0][cells(piece), :], bufs[1][cells(piece), :]], axis=1)

    def two_lines(bufs, first, second):
        return jnp.concatenate([both(bufs, first), both(bufs, second)], axis=0).astype(jnp.bfloat16)

    def pack_rows(bufs, t, h):
        h_out[t, pl.ds(h * T, 2 * T), :] = two_lines(bufs, ("H", h, 0, 3), ("H", h + 1, 0, 3))

    def pack_sends():
        for j, piece in enumerate((("H", 0, 0, 3), ("V", 0, 0, 3), ("V", 0, 22, 3), ("H", 22, 0, 3))):
            kind, h, w, n = piece
            line_send[j] = two_lines(hr, piece, (kind, h + 1, w, n) if kind == "H" else (kind, h, w + 1, n))
        for j, (h, w) in enumerate(((0, 0), (0, 22), (22, 0), (22, 22))):
            for p in range(2):
                lanes = pl.ds(p * 128, 128)
                for s in range(2):
                    cor_send[j, pl.ds(2 * s, 2), lanes] = hr[p][pl.ds(addr(h, w + s), 2, stride=2 * PITCH), :]
                cor_send[j, pl.ds(4, 1), lanes] = ce[p][pl.ds(addr(h and T - 1, w and T - 1), 1), :]
        for j, piece in enumerate((("H", 0, 0, 3), ("V", 0, 0, 3), ("V", 0, 23, 3), ("H", 23, 0, 3))):
            cline_send[j] = both(ce, piece)

    LINES = {0: 0, 1: 1, 6: 2, 7: 3}
    CORNERS = {2: 0, 3: 1, 4: 2, 5: 3}
    SENT = (cor_send, line_send, cline_send)
    LANDED = (corner, hline, cline)
    MESSAGES = [(k, 0) for k in (2, 3, 4, 5)] + [(k, n) for n in (1, 2) for k in (1, 6, 0, 7)]

    def copy(k, n, slot):
        dev, swapped = target(k)
        place = CORNERS[k] if n == 0 else LINES[k]
        there = jnp.where(swapped, 3 - place, place)
        return pltpu.make_async_remote_copy(
            src_ref=SENT[n].at[place], dst_ref=LANDED[n].at[slot, there], send_sem=send_sem.at[n],
            recv_sem=recv_sem.at[slot, n], device_id=dev, device_id_type=MESH)

    def whole(n, slot):
        return pltpu.make_async_remote_copy(
            src_ref=SENT[n], dst_ref=LANDED[n].at[slot], send_sem=send_sem.at[n],
            recv_sem=recv_sem.at[slot, n], device_id=target(0)[0], device_id_type=MESH)

    def start_sends(slot, go=None):
        for k, n in MESSAGES:
            if go is None:
                copy(k, n, slot).start()
            else:
                pl.when(go)(lambda k=k, n=n: copy(k, n, slot).start())

    def wait_sends(slot):
        for n in range(3):
            whole(n, slot).wait_send()

    def wait_recvs(slot, kinds):
        for n in kinds:
            whole(n, slot).wait_recv()

    def unpack_h(slot):
        for k in range(8):
            dr, dc = DIRS[k]
            ok = present[k] == 1
            if dr and dc:
                val = jnp.where(ok, corner[slot, CORNERS[k]], 0.0)
                h, w = (-2 if dr < 0 else T), (-2 if dc < 0 else T)
                for s in range(2):
                    for p in range(2):
                        hr[p][pl.ds(addr(h, w + s), 2, stride=2 * PITCH), :] = val[2 * s:2 * s + 2, p * 128:(p + 1) * 128]
            else:
                val = jnp.where(ok, hline[slot, LINES[k]].astype(jnp.float32), 0.0)
                for s in range(2):
                    piece = ("H", (-2 if dr < 0 else T) + s, 0, 3) if dr else ("V", 0, (-2 if dc < 0 else T) + s, 3)
                    for p in range(2):
                        hr[p][cells(piece), :] = val[s * T:(s + 1) * T, p * 128:(p + 1) * 128]

    def unpack_c(slot):
        for k in range(8):
            dr, dc = DIRS[k]
            h, w = (-1 if dr < 0 else T), (-1 if dc < 0 else T)
            for p in range(2):
                lanes = pl.ds(p * 128, 128)
                if dr and dc:
                    ce[p][pl.ds(addr(h, w), 1), :] = corner[slot, CORNERS[k], pl.ds(4, 1), lanes]
                else:
                    piece = ("H", h, 0, 3) if dr else ("V", 0, w, 3)
                    ce[p][cells(piece), :] = cline[slot, LINES[k], :, lanes]

    pack_sends()
    pl.semaphore_wait(barrier, 8)
    start_sends(0)
    for ld in loads:
        ld.wait()

    def rhs(p, k):
        parts = [wts[p, tap, pl.ds(half * 128, 128), :] for tap, half in KTILES[k]]
        return jnp.concatenate(parts, axis=0)

    def lhs_of(bufs, block, k):
        parts = []
        for tap, half in KTILES[k]:
            dh, dw = TAPS[tap]
            parts.append(jnp.concatenate([bufs[half][cells(piece, dh, dw), :] for piece in block], axis=0))
        return jnp.concatenate(parts, axis=1).astype(jnp.bfloat16)

    def epilogue(i, p, pair, gates, c_src, c_dst, h_dst, step_bias, rim):
        b_i, b_f, b_o, b_g = (step_bias[gate * 2 + p] for gate in range(4))
        for s, piece in enumerate(pair):
            v = gates[16 * i + 8 * s:16 * i + 8 * s + 8]
            in_gate = 0.5 * jnp.tanh(0.5 * (v[:, :128] + b_i)) + 0.5
            forget = 0.5 * jnp.tanh(0.5 * (v[:, 128:256] + b_f)) + 0.5
            out_gate = 0.5 * jnp.tanh(0.5 * (v[:, 256:384] + b_o)) + 0.5
            cand = jnp.tanh(v[:, 384:] + b_g)
            c_new = forget * c_src[p][cells(piece), :] + in_gate * cand
            c_dst[p][cells(piece), :] = c_new
            h_new = (out_gate * jnp.tanh(c_new)).astype(jnp.bfloat16).astype(jnp.float32)
            if rim == 1:
                h_new = h_new * mask[cells(piece), :]
            h_dst[p][cells(piece), :] = h_new
            if rim == 2 and (piece[0] == "V" or piece[1] in (0, 1, 22, 23) or piece[2] in (0, 16)):
                hr[p][cells(piece), :] = h_new

    def trip_steps(trip, _):
        todo = []
        for u in range(UNROLL):
            todo = pair_steps(trip * UNROLL + u, u % 2 if UNROLL % 2 == 0 else lax.rem(trip * UNROLL + u, 2), u == UNROLL - 1, todo)
        for unit in todo:
            unit()
        return 0

    def pair_steps(n, slot, may_end, todo):
        biases = []
        for s in range(2):
            line = bias[pl.ds(2 * n + s, 1), :]
            biases.append([jnp.broadcast_to(line[:, j * 128:(j + 1) * 128], (8, 128)) for j in range(8)])
        first = (ho, ce, co, biases[0])
        second = (he, co, ce, biases[1])
        plan = [(IN1, he, first, 0), (RIM1, hr, first, 1), (RIM2, ho, second, 2), (IN2, ho, second, 0)]
        for b, p in ((b, p) for b in range(4) for p in range(2)):
            block, src, (h_dst, c_src, c_dst, step_bias), rim = plan[b]
            groups = split8(block)
            per_tile = -(-len(todo) // 4)
            gates = None
            for k in range(9):
                part = jnp.dot(lhs_of(src, block, k), rhs(p, k), preferred_element_type=jnp.float32)
                gates = part if gates is None else gates + part
                for unit in todo[:per_tile]:
                    unit()
                todo = todo[per_tile:]
                if (b, p, k) == (0, 1, 7):
                    wait_recvs(slot, (0, 1))
                    unpack_h(slot)
                if (b, p, k) == (1, 0, 5):
                    wait_recvs(slot, (2,))
                    wait_sends(slot)
                    unpack_c(slot)
                if (b, p) == (0, 1) and k < 6:
                    for h in range(4 * k, 4 * k + 4, 2):
                        pack_rows(he, lax.rem(2 * n + steps - 1, steps), h)
                if (b, p) == (2, 1) and k >= 3:
                    for h in range(4 * (k - 3), min(4 * (k - 3) + 4, T), 2):
                        pack_rows(ho, 2 * n, h)
                if (b, p, k) == (3, 0, 4):
                    pack_sends()
                    start_sends(1 - slot, (n < steps // 2 - 1) if may_end else None)
            todo = [functools.partial(epilogue, i, p, groups[2 * i:2 * i + 2], gates, c_src, c_dst, h_dst, step_bias, rim)
                    for i in range(len(groups) // 2)]
        return todo

    lax.fori_loop(0, steps // 2 // UNROLL, trip_steps, 0)

    for h in range(0, T, 2):
        pack_rows(he, steps - 1, h)
    for h in range(T):
        c_out[pl.ds(h * T, T), :] = both(ce, ("H", h, 0, 3))


def solution(mesh):
    row_count = mesh.shape["rows"]
    col_count = mesh.shape["cols"]
    assert mesh.shape["dp"] == 2

    def device_fn(h_init, c_init, w_rec, gate_bias):
        steps = gate_bias.shape[0]
        assert h_init.shape == (1, T, T, CH) and steps % 2 == 0
        cell_rows = 2 * ROWS * PITCH
        f32, bf16 = jnp.float32, jnp.bfloat16
        plane = [pltpu.VMEM((cell_rows, 128), f32)] * 2
        hbm = pl.BlockSpec(memory_space=pltpu.HBM)
        vmem = pl.BlockSpec(memory_space=pltpu.VMEM)
        scratch = [
            plane, plane, plane, plane, plane,
            pltpu.VMEM((cell_rows, 128), f32),
            pltpu.VMEM((2, 9, 256, 512), bf16),
            pltpu.VMEM((steps, 4 * CH), f32),
            pltpu.VMEM((T * T, CH), bf16),
            pltpu.VMEM((T * T, CH), f32),
            pltpu.VMEM((4, 2 * T, CH), bf16),
            pltpu.VMEM((4, T, CH), f32),
            pltpu.VMEM((4, 8, CH), f32),
            pltpu.VMEM((2, 4, 2 * T, CH), bf16),
            pltpu.VMEM((2, 4, T, CH), f32),
            pltpu.VMEM((2, 4, 8, CH), f32),
            pltpu.SemaphoreType.DMA((11,)),
            pltpu.SemaphoreType.DMA((3,)),
            pltpu.SemaphoreType.DMA((2, 3)),
        ]
        flat, shapes = [], []
        for s in scratch:
            shapes.append(len(s) if isinstance(s, list) else 0)
            flat += s if isinstance(s, list) else [s]

        def body(*refs):
            args, rest = refs[:6], list(refs[6:])
            grouped = []
            for count in shapes:
                if count:
                    grouped.append([rest.pop(0) for _ in range(count)])
                else:
                    grouped.append(rest.pop(0))
            kernel(steps, row_count, col_count, *args, *grouped)

        h_seq, c_last = pl.pallas_call(
            body,
            out_shape=(jax.ShapeDtypeStruct((steps, T * T, CH), bf16), jax.ShapeDtypeStruct((T * T, CH), f32)),
            in_specs=[hbm] * 4,
            out_specs=(vmem, vmem),
            scratch_shapes=flat,
            compiler_params=pltpu.CompilerParams(
                collective_id=0, has_side_effects=True, vmem_limit_bytes=40 * 1024 * 1024),
            name="conv_lstm",
        )(*(pltpu.with_memory_space_constraint(x, pltpu.HBM) for x in (h_init.reshape(T * T, CH), c_init.reshape(T * T, CH), w_rec.reshape(9, CH, 4 * CH), gate_bias)))
        return h_seq.reshape(steps, 1, T, T, CH), c_last.reshape(1, T, T, CH)

    state_spec = P("dp", "rows", "cols", None)
    return jax.shard_map(device_fn, mesh=mesh, in_specs=(state_spec, state_spec, P(), P()), out_specs=(P(None, "dp", "rows", "cols", None), state_spec), check_vma=False)
```

```python
import functools

import jax
import jax.numpy as jnp
from jax import lax
from jax.experimental import pallas as pl
from jax.experimental.pallas import tpu as pltpu
from jax.sharding import PartitionSpec as P

T = 24
CH = 256
PITCH = 29
ROWS = 34
LAST = 12
UNROLL = 2
MESH = pl.DeviceIdType.MESH
DIRS = ((-1, 0), (0, -1), (-1, -1), (-1, 1), (1, -1), (1, 1), (0, 1), (1, 0))


def addr(h, w):
    return 2 * ((h + 2) * PITCH + (w + 2))


def cells(piece, dh=0, dw=0):
    kind, h, w, n = piece
    stride = 2 if kind == "H" else 2 * PITCH
    return pl.ds(addr(h + dh, w + dw), 8 * n, stride=stride)


IN1 = [("V", 1, w, 2) for w in range(1, 23)] + [p for h in range(17, 23) for p in (("H", h, 1, 2), ("H", h, 15, 1))]
RIM1 = [("V", 1, w, 3) for w in (-1, 0, 23, 24)]
RIM1 += [p for h in (-1, 0) for p in (("H", h, -1, 3), ("H", h, 17, 1))]
RIM1 += [p for h in (23, 24) for p in (("H", h, 1, 2), ("H", h, 15, 1))]
RIM2 = [("H", h, 0, 3) for h in (0, 1, 18, 19, 20, 21, 22, 23)] + [("V", 2, w, 2) for w in (0, 1, 22, 23)]
IN2 = [("V", 2, w, 2) for w in range(2, 22)]

TAPS = [(dh, dw) for dh in (-1, 0, 1) for dw in (-1, 0, 1)]
KTILES = [((2 * k, 0), (2 * k + 1, 0)) for k in range(4)] + [((8, 0), (8, 1))]
KTILES += [((2 * k, 1), (2 * k + 1, 1)) for k in range(4)]


def split8(block):
    out = []
    for kind, h, w, n in block:
        for g in range(n):
            out.append((kind, h + 8 * g, w, 1) if kind == "V" else (kind, h, w + 8 * g, 1))
    return out


def kernel(steps, row_count, col_count, h_in, c_in, w_in, bias_in, h_out, c_out, *scratch):
    (he, hr, ho, ce, co, mask, wts, bias, h_stage, c_stage, line_send, cline_send, cor_send,
     hline, cline, corner, load_sem, send_sem, recv_sem) = scratch
    dp = lax.axis_index("dp")
    col = lax.axis_index("cols")
    row = lax.axis_index("rows")

    def has(k):
        dr, dc = DIRS[k]
        ok = jnp.int32(1)
        if dr:
            ok = ok * jnp.where((row > 0) if dr < 0 else (row < row_count - 1), 1, 0)
        if dc:
            ok = ok * jnp.where((col > 0) if dc < 0 else (col < col_count - 1), 1, 0)
        return ok

    present = [has(k) for k in range(8)]

    def target(k):
        dr, dc = DIRS[k]
        ok = present[k]
        return (jnp.where(ok == 1, dp, 1 - dp), col + ok * dc, row + ok * dr), ok == 1

    loads = []
    for p in range(2):
        for gate in range(4):
            loads.append(pltpu.make_async_copy(
                w_in.at[:, :, pl.ds(gate * CH + p * 128, 128)],
                wts.at[p, :, :, pl.ds(gate * 128, 128)], load_sem.at[2 + p * 4 + gate]))
    h_load = pltpu.make_async_copy(h_in, h_stage, load_sem.at[0])
    c_load = pltpu.make_async_copy(c_in, c_stage, load_sem.at[1])
    loads.append(pltpu.make_async_copy(bias_in, bias, load_sem.at[10]))
    h_load.start()
    c_load.start()
    for ld in loads:
        ld.start()

    barrier = pltpu.get_barrier_semaphore()
    for k in range(8):
        dev, _ = target(k)
        pl.semaphore_signal(barrier, inc=1, device_id=dev, device_id_type=MESH)

    hmin, hmax = -present[0], T - 1 + present[7]
    wmin, wmax = -present[1], T - 1 + present[6]
    for piece in split8(RIM1):
        kind, h, w, _ = piece
        line = lax.broadcasted_iota(jnp.int32, (8, 128), 0)
        hh = line + h if kind == "V" else jnp.full((8, 128), h, jnp.int32)
        ww = line + w if kind == "H" else jnp.full((8, 128), w, jnp.int32)
        inside = (hh >= hmin) & (hh <= hmax) & (ww >= wmin) & (ww <= wmax)
        mask[cells(piece), :] = jnp.where(inside, 1.0, 0.0)

    h_load.wait()
    for h in range(0, T, 2):
        val = h_stage[pl.ds(h * T, 2 * T), :].astype(jnp.float32)
        for s in range(2):
            for p in range(2):
                part = val[s * T:(s + 1) * T, p * 128:(p + 1) * 128]
                he[p][cells(("H", h + s, 0, 3)), :] = part
                hr[p][cells(("H", h + s, 0, 3)), :] = part
    c_load.wait()
    for h in range(T):
        for p in range(2):
            ce[p][cells(("H", h, 0, 3)), :] = c_stage[pl.ds(h * T, T), pl.ds(p * 128, 128)]

    def both(bufs, piece):
        return jnp.concatenate([bufs[0][cells(piece), :], bufs[1][cells(piece), :]], axis=1)

    def two_lines(bufs, first, second):
        return jnp.concatenate([both(bufs, first), both(bufs, second)], axis=0).astype(jnp.bfloat16)

    def pack_rows(bufs, t, h):
        h_out[t, pl.ds(h * T, 2 * T), :] = two_lines(bufs, ("H", h, 0, 3), ("H", h + 1, 0, 3))

    def pack_sends():
        for j, piece in enumerate((("H", 0, 0, 3), ("V", 0, 0, 3), ("V", 0, 22, 3), ("H", 22, 0, 3))):
            kind, h, w, n = piece
            line_send[j] = two_lines(hr, piece, (kind, h + 1, w, n) if kind == "H" else (kind, h, w + 1, n))
        for j, (h, w) in enumerate(((0, 0), (0, 22), (22, 0), (22, 22))):
            for p in range(2):
                lanes = pl.ds(p * 128, 128)
                for s in range(2):
                    cor_send[j, pl.ds(2 * s, 2), lanes] = hr[p][pl.ds(addr(h, w + s), 2, stride=2 * PITCH), :]
                cor_send[j, pl.ds(4, 1), lanes] = ce[p][pl.ds(addr(h and T - 1, w and T - 1), 1), :]
        for j, piece in enumerate((("H", 0, 0, 3), ("V", 0, 0, 3), ("V", 0, 23, 3), ("H", 23, 0, 3))):
            cline_send[j] = both(ce, piece)

    LINES = {0: 0, 1: 1, 6: 2, 7: 3}
    CORNERS = {2: 0, 3: 1, 4: 2, 5: 3}
    SENT = (cor_send, line_send, cline_send)
    LANDED = (corner, hline, cline)
    MESSAGES = [(k, 0) for k in (2, 3, 4, 5)] + [(k, n) for n in (1, 2) for k in (1, 6, 0, 7)]

    def copy(k, n, slot):
        dev, swapped = target(k)
        place = CORNERS[k] if n == 0 else LINES[k]
        there = jnp.where(swapped, 3 - place, place)
        return pltpu.make_async_remote_copy(
            src_ref=SENT[n].at[place], dst_ref=LANDED[n].at[slot, there], send_sem=send_sem.at[n],
            recv_sem=recv_sem.at[slot, n], device_id=dev, device_id_type=MESH)

    def whole(n, slot):
        return pltpu.make_async_remote_copy(
            src_ref=SENT[n], dst_ref=LANDED[n].at[slot], send_sem=send_sem.at[n],
            recv_sem=recv_sem.at[slot, n], device_id=target(0)[0], device_id_type=MESH)

    def start_sends(slot, go=None):
        for k, n in MESSAGES:
            if go is None:
                copy(k, n, slot).start()
            else:
                pl.when(go)(lambda k=k, n=n: copy(k, n, slot).start())

    def wait_sends(slot):
        for n in range(3):
            whole(n, slot).wait_send()

    def wait_recvs(slot, kinds):
        for n in kinds:
            whole(n, slot).wait_recv()

    def unpack_h(slot):
        for k in range(8):
            dr, dc = DIRS[k]
            ok = present[k] == 1
            if dr and dc:
                val = jnp.where(ok, corner[slot, CORNERS[k]], 0.0)
                h, w = (-2 if dr < 0 else T), (-2 if dc < 0 else T)
                for s in range(2):
                    for p in range(2):
                        hr[p][pl.ds(addr(h, w + s), 2, stride=2 * PITCH), :] = val[2 * s:2 * s + 2, p * 128:(p + 1) * 128]
            else:
                val = jnp.where(ok, hline[slot, LINES[k]].astype(jnp.float32), 0.0)
                for s in range(2):
                    piece = ("H", (-2 if dr < 0 else T) + s, 0, 3) if dr else ("V", 0, (-2 if dc < 0 else T) + s, 3)
                    for p in range(2):
                        hr[p][cells(piece), :] = val[s * T:(s + 1) * T, p * 128:(p + 1) * 128]

    def unpack_c(slot):
        for k in range(8):
            dr, dc = DIRS[k]
            h, w = (-1 if dr < 0 else T), (-1 if dc < 0 else T)
            for p in range(2):
                lanes = pl.ds(p * 128, 128)
                if dr and dc:
                    ce[p][pl.ds(addr(h, w), 1), :] = corner[slot, CORNERS[k], pl.ds(4, 1), lanes]
                else:
                    piece = ("H", h, 0, 3) if dr else ("V", 0, w, 3)
                    ce[p][cells(piece), :] = cline[slot, LINES[k], :, lanes]

    pack_sends()
    pl.semaphore_wait(barrier, 8)
    start_sends(0)
    for ld in loads:
        ld.wait()

    def rhs(p, k):
        parts = [wts[p, tap, pl.ds(half * 128, 128), :] for tap, half in KTILES[k]]
        return jnp.concatenate(parts, axis=0)

    def lhs_of(bufs, block, k):
        parts = []
        for tap, half in KTILES[k]:
            dh, dw = TAPS[tap]
            parts.append(jnp.concatenate([bufs[half][cells(piece, dh, dw), :] for piece in block], axis=0))
        return jnp.concatenate(parts, axis=1).astype(jnp.bfloat16)

    def epilogue(at, p, piece, gates, c_src, c_dst, h_dst, step_bias, rim):
        kind, h, w, n = piece
        v = gates[at:at + 8 * n]
        in_gate, forget, out_gate = (
            0.5 * jnp.tanh(0.5 * (v[:, j * 128:(j + 1) * 128] + step_bias[2 * j + p])) + 0.5 for j in range(3))
        c_new = forget * c_src[p][cells(piece), :] + in_gate * jnp.tanh(v[:, 384:] + step_bias[6 + p])
        c_dst[p][cells(piece), :] = c_new
        h_new = (out_gate * jnp.tanh(c_new)).astype(jnp.bfloat16).astype(jnp.float32)
        if rim == 1:
            h_new = h_new * mask[cells(piece), :]
        h_dst[p][cells(piece), :] = h_new
        if rim == 2:
            hr[p][cells(piece), :] = h_new

    def trip_steps(trip, _):
        todo = []
        for u in range(UNROLL):
            todo = pair_steps(trip * UNROLL + u, u % 2 if UNROLL % 2 == 0 else lax.rem(trip * UNROLL + u, 2), u == UNROLL - 1, todo)
        for unit in todo:
            unit()
        return 0

    def pair_steps(n, slot, may_end, todo):
        biases = []
        for s in range(2):
            line = bias[pl.ds(2 * n + s, 1), :]
            biases.append([line[:, j * 128:(j + 1) * 128] for j in range(8)])
        first = (ho, ce, co, biases[0])
        second = (he, co, ce, biases[1])
        plan = [(IN1, he, first, 0), (RIM1, hr, first, 1), (RIM2, ho, second, 2), (IN2, ho, second, 0)]
        for b, p in ((0, 0), (0, 1), (1, 0), (1, 1), (2, 0), (2, 1), (3, 0), (3, 1), (4, 1)):
            block, src, (h_dst, c_src, c_dst, step_bias), rim = plan[min(b, 3)]
            if (b, p) == (3, 1):
                block = block[:LAST]
            if b == 4:
                block = block[LAST:]
            per_tile = -(-len(todo) // 4)
            gates = None
            for k in range(9):
                part = jnp.dot(lhs_of(src, block, k), rhs(p, k), preferred_element_type=jnp.float32)
                gates = part if gates is None else gates + part
                for unit in todo[:per_tile]:
                    unit()
                todo = todo[per_tile:]
                if (b, p, k) == (0, 1, 7):
                    wait_recvs(slot, (0, 1))
                    unpack_h(slot)
                if (b, p, k) == (1, 0, 5):
                    wait_recvs(slot, (2,))
                    wait_sends(slot)
                    unpack_c(slot)
                if (b, p) == (0, 1) and k < 6:
                    for h in range(4 * k, 4 * k + 4, 2):
                        pack_rows(he, lax.rem(2 * n + steps - 1, steps), h)
                if (b, p) == (2, 1) and k >= 3:
                    for h in range(4 * (k - 3), min(4 * (k - 3) + 4, T), 2):
                        pack_rows(ho, 2 * n, h)
                if (b, p, k) == (3, 0, 4):
                    pack_sends()
                    start_sends(1 - slot, (n < steps // 2 - 1) if may_end else None)
            todo, at = [], 0
            for piece in block:
                todo.append(functools.partial(epilogue, at, p, piece, gates, c_src, c_dst, h_dst, step_bias, rim))
                at += 8 * piece[3]
        return todo

    lax.fori_loop(0, steps // 2 // UNROLL, trip_steps, 0)

    for h in range(0, T, 2):
        pack_rows(he, steps - 1, h)
    for h in range(T):
        c_out[pl.ds(h * T, T), :] = both(ce, ("H", h, 0, 3))


def solution(mesh):
    row_count = mesh.shape["rows"]
    col_count = mesh.shape["cols"]
    assert mesh.shape["dp"] == 2

    def device_fn(h_init, c_init, w_rec, gate_bias):
        steps = gate_bias.shape[0]
        assert h_init.shape == (1, T, T, CH) and steps % 2 == 0
        cell_rows = 2 * ROWS * PITCH
        f32, bf16 = jnp.float32, jnp.bfloat16
        plane = [pltpu.VMEM((cell_rows, 128), f32)] * 2
        hbm = pl.BlockSpec(memory_space=pltpu.HBM)
        vmem = pl.BlockSpec(memory_space=pltpu.VMEM)
        scratch = [
            plane, plane, plane, plane, plane,
            pltpu.VMEM((cell_rows, 128), f32),
            pltpu.VMEM((2, 9, 256, 512), bf16),
            pltpu.VMEM((steps, 4 * CH), f32),
            pltpu.VMEM((T * T, CH), bf16),
            pltpu.VMEM((T * T, CH), f32),
            pltpu.VMEM((4, 2 * T, CH), bf16),
            pltpu.VMEM((4, T, CH), f32),
            pltpu.VMEM((4, 8, CH), f32),
            pltpu.VMEM((2, 4, 2 * T, CH), bf16),
            pltpu.VMEM((2, 4, T, CH), f32),
            pltpu.VMEM((2, 4, 8, CH), f32),
            pltpu.SemaphoreType.DMA((11,)),
            pltpu.SemaphoreType.DMA((3,)),
            pltpu.SemaphoreType.DMA((2, 3)),
        ]
        flat, shapes = [], []
        for s in scratch:
            shapes.append(len(s) if isinstance(s, list) else 0)
            flat += s if isinstance(s, list) else [s]

        def body(*refs):
            args, rest = refs[:6], list(refs[6:])
            grouped = []
            for count in shapes:
                if count:
                    grouped.append([rest.pop(0) for _ in range(count)])
                else:
                    grouped.append(rest.pop(0))
            kernel(steps, row_count, col_count, *args, *grouped)

        h_seq, c_last = pl.pallas_call(
            body,
            out_shape=(jax.ShapeDtypeStruct((steps, T * T, CH), bf16), jax.ShapeDtypeStruct((T * T, CH), f32)),
            in_specs=[hbm] * 4,
            out_specs=(vmem, vmem),
            scratch_shapes=flat,
            compiler_params=pltpu.CompilerParams(
                collective_id=0, has_side_effects=True, vmem_limit_bytes=40 * 1024 * 1024),
            name="conv_lstm",
        )(*(pltpu.with_memory_space_constraint(x, pltpu.HBM) for x in (h_init.reshape(T * T, CH), c_init.reshape(T * T, CH), w_rec.reshape(9, CH, 4 * CH), gate_bias)))
        return h_seq.reshape(steps, 1, T, T, CH), c_last.reshape(1, T, T, CH)

    state_spec = P("dp", "rows", "cols", None)
    return jax.shard_map(device_fn, mesh=mesh, in_specs=(state_spec, state_spec, P(), P()), out_specs=(P(None, "dp", "rows", "cols", None), state_spec), check_vma=False)
```

```python
import functools

import jax
import jax.numpy as jnp
from jax import lax
from jax.experimental import pallas as pl
from jax.experimental.pallas import tpu as pltpu
from jax.sharding import PartitionSpec as P

T = 24
CH = 256
PITCH = 29
ROWS = 34
LAST = 12
UNROLL = 2
MESH = pl.DeviceIdType.MESH
DIRS = ((-1, 0), (0, -1), (-1, -1), (-1, 1), (1, -1), (1, 1), (0, 1), (1, 0))


def addr(h, w):
    return 2 * ((h + 2) * PITCH + (w + 2))


def cells(piece, dh=0, dw=0):
    kind, h, w, n = piece
    stride = 2 if kind == "H" else 2 * PITCH
    return pl.ds(addr(h + dh, w + dw), 8 * n, stride=stride)


IN1 = [("V", 1, w, 2) for w in range(1, 23)] + [p for h in range(17, 23) for p in (("H", h, 1, 2), ("H", h, 15, 1))]
RIM1 = [("V", 1, w, 3) for w in (-1, 0, 23, 24)]
RIM1 += [p for h in (-1, 0) for p in (("H", h, -1, 3), ("H", h, 17, 1))]
RIM1 += [p for h in (23, 24) for p in (("H", h, 1, 2), ("H", h, 15, 1))]
RIM2 = [("H", h, 0, 3) for h in (0, 1, 18, 19, 20, 21, 22, 23)] + [("V", 2, w, 2) for w in (0, 1, 22, 23)]
IN2 = [("V", 2, w, 2) for w in range(2, 22)]

TAPS = [(dh, dw) for dh in (-1, 0, 1) for dw in (-1, 0, 1)]
KTILES = [((2 * k, 0), (2 * k + 1, 0)) for k in range(4)] + [((8, 0), (8, 1))]
KTILES += [((2 * k, 1), (2 * k + 1, 1)) for k in range(4)]


def split8(block):
    out = []
    for kind, h, w, n in block:
        for g in range(n):
            out.append((kind, h + 8 * g, w, 1) if kind == "V" else (kind, h, w + 8 * g, 1))
    return out


def kernel(steps, row_count, col_count, h_in, c_in, w_in, bias_in, h_out, c_out, *scratch):
    (he, hr, ho, ce, co, mask, wts, bias, h_stage, c_stage, line_send, cline_send, cor_send,
     hline, cline, corner, load_sem, send_sem, recv_sem) = scratch
    dp = lax.axis_index("dp")
    col = lax.axis_index("cols")
    row = lax.axis_index("rows")

    def has(k):
        dr, dc = DIRS[k]
        ok = jnp.int32(1)
        if dr:
            ok = ok * jnp.where((row > 0) if dr < 0 else (row < row_count - 1), 1, 0)
        if dc:
            ok = ok * jnp.where((col > 0) if dc < 0 else (col < col_count - 1), 1, 0)
        return ok

    present = [has(k) for k in range(8)]

    def target(k):
        dr, dc = DIRS[k]
        ok = present[k]
        return (jnp.where(ok == 1, dp, 1 - dp), col + ok * dc, row + ok * dr), ok == 1

    loads = []
    for p in range(2):
        for gate in range(4):
            loads.append(pltpu.make_async_copy(
                w_in.at[:, :, pl.ds(gate * CH + p * 128, 128)],
                wts.at[p, :, :, pl.ds(gate * 128, 128)], load_sem.at[2 + p * 4 + gate]))
    h_load = pltpu.make_async_copy(h_in, h_stage, load_sem.at[0])
    c_load = pltpu.make_async_copy(c_in, c_stage, load_sem.at[1])
    loads.append(pltpu.make_async_copy(bias_in, bias, load_sem.at[10]))
    h_load.start()
    c_load.start()
    for ld in loads:
        ld.start()

    barrier = pltpu.get_barrier_semaphore()
    for k in range(8):
        dev, _ = target(k)
        pl.semaphore_signal(barrier, inc=1, device_id=dev, device_id_type=MESH)

    hmin, hmax = -present[0], T - 1 + present[7]
    wmin, wmax = -present[1], T - 1 + present[6]
    for piece in split8(RIM1):
        kind, h, w, _ = piece
        line = lax.broadcasted_iota(jnp.int32, (8, 128), 0)
        hh = line + h if kind == "V" else jnp.full((8, 128), h, jnp.int32)
        ww = line + w if kind == "H" else jnp.full((8, 128), w, jnp.int32)
        inside = (hh >= hmin) & (hh <= hmax) & (ww >= wmin) & (ww <= wmax)
        mask[cells(piece), :] = jnp.where(inside, 1.0, 0.0)

    h_load.wait()
    for h in range(0, T, 2):
        val = h_stage[pl.ds(h * T, 2 * T), :].astype(jnp.float32)
        for s in range(2):
            for p in range(2):
                part = val[s * T:(s + 1) * T, p * 128:(p + 1) * 128]
                he[p][cells(("H", h + s, 0, 3)), :] = part
                hr[p][cells(("H", h + s, 0, 3)), :] = part
    c_load.wait()
    for h in range(T):
        for p in range(2):
            ce[p][cells(("H", h, 0, 3)), :] = c_stage[pl.ds(h * T, T), pl.ds(p * 128, 128)]

    def both(bufs, piece):
        return jnp.concatenate([bufs[0][cells(piece), :], bufs[1][cells(piece), :]], axis=1)

    def two_lines(bufs, first, second):
        return jnp.concatenate([both(bufs, first), both(bufs, second)], axis=0).astype(jnp.bfloat16)

    def pack_rows(bufs, t, h):
        h_out[t, pl.ds(h * T, 2 * T), :] = two_lines(bufs, ("H", h, 0, 3), ("H", h + 1, 0, 3))

    def pack_sends():
        for j, piece in enumerate((("H", 0, 0, 3), ("V", 0, 0, 3), ("V", 0, 22, 3), ("H", 22, 0, 3))):
            kind, h, w, n = piece
            line_send[j] = two_lines(hr, piece, (kind, h + 1, w, n) if kind == "H" else (kind, h, w + 1, n))
        for j, (h, w) in enumerate(((0, 0), (0, 22), (22, 0), (22, 22))):
            for p in range(2):
                lanes = pl.ds(p * 128, 128)
                for s in range(2):
                    cor_send[j, pl.ds(2 * s, 2), lanes] = hr[p][pl.ds(addr(h, w + s), 2, stride=2 * PITCH), :]
                cor_send[j, pl.ds(4, 1), lanes] = ce[p][pl.ds(addr(h and T - 1, w and T - 1), 1), :]
        for j, piece in enumerate((("H", 0, 0, 3), ("V", 0, 0, 3), ("V", 0, 23, 3), ("H", 23, 0, 3))):
            cline_send[j] = both(ce, piece)

    LINES = {0: 0, 1: 1, 6: 2, 7: 3}
    CORNERS = {2: 0, 3: 1, 4: 2, 5: 3}
    SENT = (cor_send, line_send, cline_send)
    LANDED = (corner, hline, cline)
    MESSAGES = [(k, 0) for k in (2, 3, 4, 5)] + [(k, n) for n in (1, 2) for k in (1, 6, 0, 7)]

    def copy(k, n, slot):
        dev, swapped = target(k)
        place = CORNERS[k] if n == 0 else LINES[k]
        there = jnp.where(swapped, 3 - place, place)
        return pltpu.make_async_remote_copy(
            src_ref=SENT[n].at[place], dst_ref=LANDED[n].at[slot, there], send_sem=send_sem.at[n],
            recv_sem=recv_sem.at[slot, n], device_id=dev, device_id_type=MESH)

    def whole(n, slot):
        return pltpu.make_async_remote_copy(
            src_ref=SENT[n], dst_ref=LANDED[n].at[slot], send_sem=send_sem.at[n],
            recv_sem=recv_sem.at[slot, n], device_id=target(0)[0], device_id_type=MESH)

    def start_sends(slot, go=None):
        for k, n in MESSAGES:
            if go is None:
                copy(k, n, slot).start()
            else:
                pl.when(go)(lambda k=k, n=n: copy(k, n, slot).start())

    def wait_sends(slot):
        for n in range(3):
            whole(n, slot).wait_send()

    def wait_recvs(slot, kinds):
        for n in kinds:
            whole(n, slot).wait_recv()

    def unpack_h(slot):
        for k in range(8):
            dr, dc = DIRS[k]
            ok = present[k] == 1
            if dr and dc:
                val = jnp.where(ok, corner[slot, CORNERS[k]], 0.0)
                h, w = (-2 if dr < 0 else T), (-2 if dc < 0 else T)
                for s in range(2):
                    for p in range(2):
                        hr[p][pl.ds(addr(h, w + s), 2, stride=2 * PITCH), :] = val[2 * s:2 * s + 2, p * 128:(p + 1) * 128]
            else:
                val = jnp.where(ok, hline[slot, LINES[k]].astype(jnp.float32), 0.0)
                for s in range(2):
                    piece = ("H", (-2 if dr < 0 else T) + s, 0, 3) if dr else ("V", 0, (-2 if dc < 0 else T) + s, 3)
                    for p in range(2):
                        hr[p][cells(piece), :] = val[s * T:(s + 1) * T, p * 128:(p + 1) * 128]

    def unpack_c(slot):
        for k in range(8):
            dr, dc = DIRS[k]
            h, w = (-1 if dr < 0 else T), (-1 if dc < 0 else T)
            for p in range(2):
                lanes = pl.ds(p * 128, 128)
                if dr and dc:
                    ce[p][pl.ds(addr(h, w), 1), :] = corner[slot, CORNERS[k], pl.ds(4, 1), lanes]
                else:
                    piece = ("H", h, 0, 3) if dr else ("V", 0, w, 3)
                    ce[p][cells(piece), :] = cline[slot, LINES[k], :, lanes]

    pack_sends()
    pl.semaphore_wait(barrier, 8)
    start_sends(0)
    for ld in loads:
        ld.wait()

    def rhs(p, k):
        parts = [wts[p, tap, pl.ds(half * 128, 128), :] for tap, half in KTILES[k]]
        return jnp.concatenate(parts, axis=0)

    def lhs_of(bufs, block, k):
        parts = []
        for tap, half in KTILES[k]:
            dh, dw = TAPS[tap]
            parts.append(jnp.concatenate([bufs[half][cells(piece, dh, dw), :] for piece in block], axis=0))
        return jnp.concatenate(parts, axis=1).astype(jnp.bfloat16)

    def epilogue(at, p, piece, gates, c_src, c_dst, h_dst, step_bias, rim):
        kind, h, w, n = piece
        v = gates[at:at + 8 * n]
        in_gate, forget, out_gate = (
            0.5 * jnp.tanh(0.5 * (v[:, j * 128:(j + 1) * 128] + step_bias[2 * j + p])) + 0.5 for j in range(3))
        c_new = forget * c_src[p][cells(piece), :] + in_gate * jnp.tanh(v[:, 384:] + step_bias[6 + p])
        c_dst[p][cells(piece), :] = c_new
        h_new = (out_gate * jnp.tanh(c_new)).astype(jnp.bfloat16).astype(jnp.float32)
        if rim == 1:
            h_new = h_new * mask[cells(piece), :]
        h_dst[p][cells(piece), :] = h_new
        if rim == 2:
            hr[p][cells(piece), :] = h_new

    def trip_steps(trip, _):
        todo = []
        for u in range(UNROLL):
            todo = pair_steps(trip * UNROLL + u, u % 2 if UNROLL % 2 == 0 else lax.rem(trip * UNROLL + u, 2), u == UNROLL - 1, todo)
        for unit in todo:
            unit()
        return 0

    def pair_steps(n, slot, may_end, todo):
        biases = []
        for s in range(2):
            line = bias[pl.ds(2 * n + s, 1), :]
            biases.append([line[:, j * 128:(j + 1) * 128] for j in range(8)])
        first = (ho, ce, co, biases[0])
        second = (he, co, ce, biases[1])
        plan = [(IN1, he, first, 0), (RIM1, hr, first, 1), (RIM2, ho, second, 2), (IN2, ho, second, 0)]
        for b, p in ((0, 0), (0, 1), (1, 0), (1, 1), (2, 0), (2, 1), (3, 0), (3, 1), (4, 1)):
            block, src, (h_dst, c_src, c_dst, step_bias), rim = plan[min(b, 3)]
            if (b, p) == (3, 1):
                block = block[:LAST]
            if b == 4:
                block = block[LAST:]
            per_tile = -(-len(todo) // 4)
            gates = None
            for k in range(9):
                part = jnp.dot(lhs_of(src, block, k), rhs(p, k), preferred_element_type=jnp.float32)
                gates = part if gates is None else gates + part
                for unit in todo[:per_tile]:
                    unit()
                todo = todo[per_tile:]
                if (b, p, k) == (0, 1, 7):
                    wait_recvs(slot, (0, 1))
                    unpack_h(slot)
                if (b, p, k) == (1, 0, 5):
                    wait_recvs(slot, (2,))
                    wait_sends(slot)
                    unpack_c(slot)
                if (b, p) == (0, 1) and k < 6:
                    for h in range(4 * k, 4 * k + 4, 2):
                        pack_rows(he, lax.rem(2 * n + steps - 1, steps), h)
                if (b, p) == (2, 1) and k >= 3:
                    for h in range(4 * (k - 3), min(4 * (k - 3) + 4, T), 2):
                        pack_rows(ho, 2 * n, h)
                if (b, p, k) == (3, 0, 4):
                    pack_sends()
                    start_sends(1 - slot, (n < steps // 2 - 1) if may_end else None)
            todo, at = [], 0
            for piece in block:
                todo.append(functools.partial(epilogue, at, p, piece, gates, c_src, c_dst, h_dst, step_bias, rim))
                at += 8 * piece[3]
        return todo

    lax.fori_loop(0, steps // 2 // UNROLL, trip_steps, 0)

    for h in range(0, T, 2):
        pack_rows(he, steps - 1, h)
    for h in range(T):
        c_out[pl.ds(h * T, T), :] = both(ce, ("H", h, 0, 3))


def save(h_vmem, c_vmem, h_out, c_out, sems):
    steps = h_vmem.shape[0]
    part = steps // 4
    copies = [pltpu.make_async_copy(h_vmem.at[pl.ds(i * part, part)], h_out.at[pl.ds(i * part, part)], sems.at[i]) for i in range(4)]
    copies.append(pltpu.make_async_copy(c_vmem, c_out, sems.at[4]))
    for cp in copies:
        cp.start()
    for cp in copies:
        cp.wait()


def solution(mesh):
    row_count = mesh.shape["rows"]
    col_count = mesh.shape["cols"]
    assert mesh.shape["dp"] == 2

    def device_fn(h_init, c_init, w_rec, gate_bias):
        steps = gate_bias.shape[0]
        assert h_init.shape == (1, T, T, CH) and steps % 2 == 0
        cell_rows = 2 * ROWS * PITCH
        f32, bf16 = jnp.float32, jnp.bfloat16
        plane = [pltpu.VMEM((cell_rows, 128), f32)] * 2
        hbm = pl.BlockSpec(memory_space=pltpu.HBM)
        vmem = pl.BlockSpec(memory_space=pltpu.VMEM)
        scratch = [
            plane, plane, plane, plane, plane,
            pltpu.VMEM((cell_rows, 128), f32),
            pltpu.VMEM((2, 9, 256, 512), bf16),
            pltpu.VMEM((steps, 4 * CH), f32),
            pltpu.VMEM((T * T, CH), bf16),
            pltpu.VMEM((T * T, CH), f32),
            pltpu.VMEM((4, 2 * T, CH), bf16),
            pltpu.VMEM((4, T, CH), f32),
            pltpu.VMEM((4, 8, CH), f32),
            pltpu.VMEM((2, 4, 2 * T, CH), bf16),
            pltpu.VMEM((2, 4, T, CH), f32),
            pltpu.VMEM((2, 4, 8, CH), f32),
            pltpu.SemaphoreType.DMA((11,)),
            pltpu.SemaphoreType.DMA((3,)),
            pltpu.SemaphoreType.DMA((2, 3)),
        ]
        flat, shapes = [], []
        for s in scratch:
            shapes.append(len(s) if isinstance(s, list) else 0)
            flat += s if isinstance(s, list) else [s]

        def body(*refs):
            args, rest = refs[:6], list(refs[6:])
            grouped = []
            for count in shapes:
                if count:
                    grouped.append([rest.pop(0) for _ in range(count)])
                else:
                    grouped.append(rest.pop(0))
            kernel(steps, row_count, col_count, *args, *grouped)

        h_seq, c_last = pl.pallas_call(
            body,
            out_shape=(jax.ShapeDtypeStruct((steps, T * T, CH), bf16), jax.ShapeDtypeStruct((T * T, CH), f32)),
            in_specs=[hbm] * 4,
            out_specs=(vmem, vmem),
            scratch_shapes=flat,
            compiler_params=pltpu.CompilerParams(
                collective_id=0, has_side_effects=True, vmem_limit_bytes=40 * 1024 * 1024),
            name="conv_lstm",
        )(*(pltpu.with_memory_space_constraint(x, pltpu.HBM) for x in (h_init.reshape(T * T, CH), c_init.reshape(T * T, CH), w_rec.reshape(9, CH, 4 * CH), gate_bias)))
        h_seq, c_last = pl.pallas_call(
            save,
            out_shape=(jax.ShapeDtypeStruct((steps, T * T, CH), bf16), jax.ShapeDtypeStruct((T * T, CH), f32)),
            in_specs=[vmem, vmem],
            out_specs=(hbm, hbm),
            scratch_shapes=[pltpu.SemaphoreType.DMA((5,))],
            compiler_params=pltpu.CompilerParams(vmem_limit_bytes=40 * 1024 * 1024),
            name="save",
        )(h_seq, c_last)
        return h_seq.reshape(steps, 1, T, T, CH), c_last.reshape(1, T, T, CH)

    state_spec = P("dp", "rows", "cols", None)
    return jax.shard_map(device_fn, mesh=mesh, in_specs=(state_spec, state_spec, P(), P()), out_specs=(P(None, "dp", "rows", "cols", None), state_spec), check_vma=False)
```
